128 devices in a mesh: vocab: 8 (over z, core), sample: 4 (over y), prompt: 4 (over x).
Axes of the slice: x: 4, y: 4, z: 4, core: 2. Of those that a mesh axis runs over, the one named last changes fastest.
Arguments:
- hidden: bfloat16 [1024, 4608], P(('sample', 'prompt'), 'vocab'), may hold values from -12 to 12
- gain: float32 [4608], replicated, may hold values from 0.25 to 1.75
- head: bfloat16 [4608, 256000], P(None, ('vocab', 'sample', 'prompt')), may hold values from -0.25 to 0.25
- candidates: int32 [32, 16], replicated, may hold values from 0 to 255999
- row_prompt: int32 [1024], replicated, may hold values from 0 to 31, as said below
Outputs:
- log_votes: float32 [32, 16], replicated
- row_lse: float32 [1024], P(('sample', 'prompt'))
The draws below stay inside these ranges and needn't reach their ends.
Inputs may be any that keep to these rules, and one draw needn't show every extreme that they name: `row_prompt`: every prompt has at least one row; the rows of a prompt may stand anywhere among the 1024 rows.
All inputs are finite; a program needn't handle non-finite values.
Results may differ from the reference program's by a relative error of at most 0.00051.
Values may be sent and summed in bfloat16 or wider, within the bound.
No kernel may reach another device: no remote copies, remote signals or barrier semaphores. Data moves between devices by JAX's collectives and lax.ppermute only.
A program may use at most 128 MiB of HBM per device.

```python
import jax
import jax.numpy as jnp
from jax import lax

D = 4608
V_DEV = 2000
CANDS = 16
VOCAB = 256000
ROWS = 1024
PROMPTS = 32


def draw_row_prompt(key, part):
    first, second = jax.random.split(jax.random.fold_in(key, 7))
    base = jax.random.randint(first, (ROWS,), 0, PROMPTS)
    order = jax.random.permutation(second, PROMPTS)
    places = jnp.arange(ROWS)
    return jnp.where(places < PROMPTS, order[jnp.minimum(places, PROMPTS - 1)], base).astype(jnp.int32)


def place_ends(array, key, least, top_value):
    dims = array.shape
    spot = [jax.random.randint(jax.random.fold_in(key, axis), (), 0, dims[axis]) for axis in range(len(dims))]
    array = array.at[tuple(spot)].set(least)
    longest = dims.index(max(dims))
    spot[longest] = (spot[longest] + 1) % dims[longest]
    return array.at[tuple(spot)].set(top_value)


def shard_levels(own_key, shape, cuts, low, top_value):
    def one(dim, parts):
        steps = jax.random.uniform(jax.random.fold_in(jax.random.fold_in(own_key, 6), dim), (parts,), jnp.float32, low / len(cuts), top_value / len(cuts))
        return jnp.repeat(jnp.exp(steps), shape[dim] // parts).reshape((-1,) + (1,) * (len(shape) - dim - 1))

    factor_of = one(*cuts[0])
    for cut in cuts[1:]:
        factor_of = factor_of * one(*cut)
    return factor_of


def bell_draw(own_key, dims, spread, reach, pieces=(), held_as=jnp.bfloat16):
    entries = spread * jax.random.normal(own_key, dims, jnp.float32)
    if pieces:
        entries = entries * shard_levels(own_key, dims, pieces, -0.22, 0.18)
    return jnp.clip(entries, -reach, reach).astype(held_as)


def setup_inputs(seed: int = 0) -> dict:
    splits = jax.random.split(jax.random.key(seed), 6)
    hidden = bell_draw(splits[0], (ROWS, D), 2.0, 12.0, ((0, 16), (1, 8)))
    gain = jnp.clip(1.0 + 0.15 * jax.random.normal(splits[1], (D,), jnp.float32), 0.25, 1.75)
    head = bell_draw(splits[2], (D, VOCAB), (D // 9) ** -0.5, 0.25, ((1, 128),))
    candidates = place_ends(jax.random.randint(splits[3], (PROMPTS, CANDS), 0, VOCAB), jax.random.fold_in(splits[3], 1), 0, VOCAB - 1).astype(jnp.int32)
    row_prompt = draw_row_prompt(jax.random.fold_in(splits[5], 71), 0)
    return {"hidden": hidden, "gain": gain, "head": head, "candidates": candidates, "row_prompt": row_prompt}


CAP = 30.0
EPS = 1e-06

def reference(hidden, gain, head, candidates, row_prompt):
    xf = hidden.astype(jnp.float32)
    mean_sq = lax.optimization_barrier(jnp.mean(xf * xf, axis=1, keepdims=True))
    normed = (xf * lax.rsqrt(mean_sq + EPS) * gain).astype(jnp.bfloat16)
    onehot = (row_prompt[:, None] == jnp.arange(PROMPTS, dtype=jnp.int32)[None, :]).astype(jnp.float32)
    wanted = candidates[row_prompt]
    blocks = VOCAB // V_DEV

    def step(index, carry):
        total, numer = carry
        begin = (index * V_DEV).astype(jnp.int32)
        columns = lax.dynamic_slice_in_dim(head, begin, V_DEV, 1)
        logits = CAP * jnp.tanh(jnp.dot(normed, columns, preferred_element_type=jnp.float32) / CAP)
        exps = jnp.exp(logits)
        local = wanted - begin
        inside = (local >= 0) & (local < V_DEV)
        picked = jnp.take_along_axis(exps, jnp.clip(local, 0, V_DEV - 1), axis=1)
        return (total + lax.optimization_barrier(jnp.sum(exps, axis=1)), numer + jnp.where(inside, picked, jnp.zeros_like(picked)))
    start = (jnp.zeros((ROWS,), jnp.float32), jnp.zeros((ROWS, CANDS), jnp.float32))
    total, numer = lax.fori_loop(0, blocks, step, start)
    prob = numer / total[:, None]
    tally = jnp.dot(onehot.T, prob, precision=lax.Precision.HIGHEST, preferred_element_type=jnp.float32)
    return (jnp.log(tally), jnp.log(total))
```

```python
import jax
import jax.numpy as jnp
import numpy as np
from jax import lax
from jax.experimental import pallas as pl
from jax.experimental.pallas import tpu as pltpu
from jax.sharding import Mesh
from jax.sharding import PartitionSpec as P

CAP = 30.0
EPS = 1e-06
ALL = ("z", "core", "y", "x")
SWAP = [(0, 1), (1, 0)]
SHIFTS = (0, 1, 3, 2)
TILE = 400


def shift_pairs(step):
    pairs = []
    for z in range(4):
        for core in range(2):
            for y in range(4):
                for x in range(4):
                    tz, tx = (z, (x + step) % 4) if core == 0 else ((z + step) % 4, x)
                    pairs.append((((z * 2 + core) * 4 + y) * 4 + x, ((tz * 2 + core) * 4 + y) * 4 + tx))
    return pairs


def norm_kernel(raw_ref, gain_ref, out_ref):
    shards, rows, cols = raw_ref.shape
    total = jnp.zeros((rows, 1), jnp.float32)
    for k in range(shards):
        part = raw_ref[k].astype(jnp.float32)
        total = total + jnp.sum(part * part, axis=1, keepdims=True)
    scale = lax.rsqrt(total / (shards * cols) + EPS)
    for k in range(0, shards, 2):
        pair = jnp.concatenate([raw_ref[k].astype(jnp.float32), raw_ref[k + 1].astype(jnp.float32)], axis=1)
        gain = gain_ref[:, k * cols : (k + 2) * cols]
        out_ref[:, k * cols : (k + 2) * cols] = (pair * scale * gain).astype(jnp.bfloat16)


def list_kernel(cand_ref, offset_ref, out_ref):
    count = cand_ref.shape[0]
    offset = offset_ref[0]

    def step(q, found):
        local = cand_ref[q] - offset
        out_ref[found] = local * count + q
        return found + jnp.where((local >= 0) & (local < 2000), 1, 0)

    out_ref[count] = lax.fori_loop(0, count, step, jnp.int32(0), unroll=8)


def head_kernel(chunk, slot_ref, list_ref, own_ref, other_ref, prompt_ref, head_ref, out_ref, act, exps, sums, votes):
    step = pl.program_id(0)
    rows = own_ref.shape[0]

    @pl.when(step == 0)
    def _():
        act[:rows, :] = own_ref[...]
        act[rows:, :] = other_ref[...]
        sums[...] = jnp.zeros_like(sums)
        votes[...] = jnp.zeros_like(votes)

    raw = lax.dot_general(head_ref[...], act[...], (((1,), (1,)), ((), ())), preferred_element_type=jnp.float32)
    value = jnp.exp(CAP * jnp.tanh(raw / CAP))
    exps[pl.ds(pl.multiple_of(step * TILE, 8), TILE), :] = value
    sums[...] += jnp.sum(value.reshape(TILE // 8, 8, 2 * rows), axis=0)

    @pl.when(step == pl.num_programs(0) - 1)
    def _():
        prompts = jnp.concatenate(
            [prompt_ref[pl.ds(slot_ref[2 * chunk], 1), :], prompt_ref[pl.ds(slot_ref[2 * chunk + 1], 1), :]], axis=1
        )

        def vote(m, carry):
            code = list_ref[m]
            local, q = code // 512, code % 512
            row = exps[pl.ds(local, 1), :]
            spot = pl.ds(q % 16, 1)
            votes[spot, :] += jnp.where(prompts == q // 16, row, 0.0)
            return carry

        lax.fori_loop(0, list_ref[512], vote, 0)
        out_ref[:16, :] = votes[...]
        out_ref[16:, :] = jnp.broadcast_to(jnp.sum(sums[...], axis=0, keepdims=True), (8, 2 * rows))


def pack_kernel(slot_ref, a_ref, b_ref, c_ref, d_ref, out_ref, votes, totals):
    for chunk, ref in enumerate((a_ref, b_ref, c_ref, d_ref)):
        for half in range(2):
            spot = pl.ds(pl.multiple_of(slot_ref[2 * chunk + half] * 16, 8), 16)
            lanes = slice(half * 128, (half + 1) * 128)
            votes[spot, :] = ref[:16, lanes]
            totals[spot, :] = jnp.broadcast_to(ref[16:17, lanes], (16, 128))
    out_ref[:, :128] = votes[...].T
    out_ref[:, 128:] = totals[...].T


def tally_kernel(prompt_ref, group_ref, got_ref, votes_ref, lse_ref):
    prob = got_ref[:, :128]
    lane = lax.broadcasted_iota(jnp.int32, (32, 128), 1)
    which = lax.broadcasted_iota(jnp.int32, (32, 128), 0)
    picked = jnp.zeros((32, 128), jnp.float32)
    for j in range(8):
        onehot = (prompt_ref[j : j + 1, :] == which).astype(jnp.float32)
        part = jnp.dot(onehot, prob, precision=lax.Precision.HIGHEST, preferred_element_type=jnp.float32)
        picked = picked + jnp.where(lane // 16 == j, part, 0.0)
    fold = lax.broadcasted_iota(jnp.int32, (128, 16), 0) % 16 == lax.broadcasted_iota(jnp.int32, (128, 16), 1)
    tally = jnp.dot(picked, fold.astype(jnp.float32), precision=lax.Precision.HIGHEST, preferred_element_type=jnp.float32)
    votes_ref[...] = jnp.log(tally)
    mine = jnp.log(got_ref[pl.ds(pl.multiple_of(group_ref[0] * 8, 8), 8), 128:])
    sub = lax.broadcasted_iota(jnp.int32, (8, 128), 0)
    lane8 = lax.broadcasted_iota(jnp.int32, (8, 128), 1)
    spread = jnp.sum(jnp.where(lane8 % 16 == sub, mine, 0.0), axis=0, keepdims=True)
    src = lax.broadcasted_iota(jnp.int32, (128, 64), 0)
    dst = lax.broadcasted_iota(jnp.int32, (128, 64), 1)
    place = (src == (dst // 8) * 16 + dst % 8).astype(jnp.float32)
    lse_ref[...] = jnp.dot(
        jnp.broadcast_to(spread, (8, 128)), place, precision=lax.Precision.HIGHEST, preferred_element_type=jnp.float32
    )


def vmem():
    return pl.BlockSpec(memory_space=pltpu.VMEM)


def smem():
    return pl.BlockSpec(memory_space=pltpu.SMEM)


def head_call(chunk, slots, listed, own, other, prompts, head):
    rows, width = own.shape
    vocab = head.shape[0]
    whole = lambda shape: pl.BlockSpec(shape, lambda i: (0, 0))
    return pl.pallas_call(
        lambda *refs: head_kernel(chunk, *refs),
        grid=(vocab // TILE,),
        in_specs=[
            smem(),
            smem(),
            whole((rows, width)),
            whole((rows, width)),
            whole((8, 128)),
            pl.BlockSpec((TILE, width), lambda i: (i, 0)),
        ],
        out_specs=whole((24, 2 * rows)),
        out_shape=jax.ShapeDtypeStruct((24, 2 * rows), jnp.float32),
        scratch_shapes=[
            pltpu.VMEM((2 * rows, width), jnp.bfloat16),
            pltpu.VMEM((vocab, 2 * rows), jnp.float32),
            pltpu.VMEM((8, 2 * rows), jnp.float32),
            pltpu.VMEM((16, 2 * rows), jnp.float32),
        ],
        compiler_params=pltpu.CompilerParams(vmem_limit_bytes=32 * 1024 * 1024),
        cost_estimate=pl.CostEstimate(
            flops=4 * rows * width * vocab, bytes_accessed=2 * vocab * width, transcendentals=4 * rows * vocab
        ),
        name=f"head{chunk}",
    )(slots, listed, own, other, prompts, head)


def body(hidden, gain, head, candidates, row_prompt):
    width, vocab_dev = head.shape
    z, core, y, x = (lax.axis_index(name) for name in ALL)
    cols = hidden.shape[1]

    slices = hidden.reshape(8, 8, cols)
    low = jnp.broadcast_to(slices[:4].reshape(1, 1, 4, 8, cols), (4, 4, 4, 8, cols))
    high = jnp.broadcast_to(slices[4:].reshape(4, 1, 1, 8, cols), (4, 4, 4, 8, cols))
    outgoing = jnp.stack([low, high], axis=1).reshape(128, 8, cols)
    raw = lax.all_to_all(outgoing, ALL, 0, 0, tiled=True).reshape(8, 128, cols)
    normed = pl.pallas_call(
        norm_kernel,
        in_specs=[vmem(), vmem()],
        out_specs=vmem(),
        out_shape=jax.ShapeDtypeStruct((128, width), jnp.bfloat16),
        name="norm",
    )(raw, gain.reshape(1, width))

    order = jnp.arange(8, dtype=jnp.int32)
    back = jnp.asarray(np.repeat(np.array(SHIFTS, np.int32), 2))
    slots = jnp.where((order % 2) == core, (x - back) % 4, 4 + (z - back) % 4).astype(jnp.int32)
    prompts = row_prompt.reshape(16, 8, 8).transpose(1, 0, 2).reshape(8, 128)
    offset = (lax.axis_index(ALL) * vocab_dev).astype(jnp.int32).reshape(1)
    listed = pl.pallas_call(
        list_kernel,
        in_specs=[smem(), smem()],
        out_specs=smem(),
        out_shape=jax.ShapeDtypeStruct((513,), jnp.int32),
        name="listing",
    )(candidates.reshape(512), offset)

    head_t = head.T
    run = lambda chunk, own, other: head_call(chunk, slots, listed, own, other, prompts, head_t)
    plus = lax.ppermute(normed, ALL, shift_pairs(1))
    minus = lax.ppermute(normed, ALL, shift_pairs(3))
    swapped = lax.ppermute(normed, "core", SWAP)
    first = run(0, normed, swapped)
    held, first = lax.optimization_barrier((normed, first))
    far = lax.ppermute(held, ALL, shift_pairs(2))
    second = run(1, plus, lax.ppermute(plus, "core", SWAP))
    third = run(2, minus, lax.ppermute(minus, "core", SWAP))
    fourth = run(3, far, lax.ppermute(far, "core", SWAP))

    packed = pl.pallas_call(
        pack_kernel,
        in_specs=[smem(), vmem(), vmem(), vmem(), vmem()],
        out_specs=vmem(),
        out_shape=jax.ShapeDtypeStruct((128, 256), jnp.float32),
        scratch_shapes=[pltpu.VMEM((128, 128), jnp.float32), pltpu.VMEM((128, 128), jnp.float32)],
        name="pack",
    )(slots, first, second, third, fourth)
    mine = lax.all_to_all(packed.reshape(128, 1, 256), ALL, 0, 0, tiled=True).sum(axis=0)
    prob = mine[:, :128] / mine[:, 128:]
    shared = jnp.concatenate([prob, mine[:, 128:]], axis=1)
    got = lax.all_to_all(jnp.broadcast_to(shared[None], (128, 1, 256)), ALL, 0, 0, tiled=True)
    votes, lse = pl.pallas_call(
        tally_kernel,
        in_specs=[vmem(), smem(), vmem()],
        out_specs=[vmem(), vmem()],
        out_shape=[jax.ShapeDtypeStruct((32, 16), jnp.float32), jax.ShapeDtypeStruct((8, 64), jnp.float32)],
        name="tally",
    )(prompts, (y * 4 + x).astype(jnp.int32).reshape(1), got.reshape(128, 256))
    return votes, lse[0]


def solution(mesh):
    fine = Mesh(mesh.devices.reshape(4, 2, 4, 4), ALL)
    placed = (P(("y", "x"), ("z", "core")), P(), P(None, ALL), P(), P())
    return jax.shard_map(body, mesh=fine, in_specs=placed, out_specs=(P(), P(("y", "x"))), check_vma=False)
```
